8 devices in a mesh: dp: 2 (over z, y), sp: 4 (over x, core).
Axes of the slice: x: 2, y: 2, z: 1, core: 2. Of those that a mesh axis runs over, the one named last changes fastest.
Arguments:
- dec_hidden: bfloat16 [4096, 1280], P(('dp', 'sp')), parts along dimension 0
- memory: bfloat16 [4096, 1280], P(('dp', 'sp')), parts along dimension 0
- mem_len: int32 [2], P('dp'), parts along dimension 0
- gain_self: bfloat16 [2, 1280], replicated
- gain_cross: bfloat16 [2, 1280], replicated
- gain_mlp: bfloat16 [2, 1280], replicated
- self_q: bfloat16 [2, 1280, 1280], replicated
- self_k: bfloat16 [2, 1280, 1280], replicated
- self_v: bfloat16 [2, 1280, 1280], replicated
- self_o: bfloat16 [2, 1280, 1280], replicated
- cross_q: bfloat16 [2, 1280, 1280], replicated
- cross_k: bfloat16 [2, 1280, 64], replicated
- cross_v: bfloat16 [2, 1280, 64], replicated
- cross_o: bfloat16 [2, 1280, 1280], replicated
- mlp_gate: bfloat16 [2, 1280, 5120], replicated
- mlp_up: bfloat16 [2, 1280, 5120], replicated
- mlp_down: bfloat16 [2, 5120, 1280], replicated
Outputs:
- output: bfloat16 [4096, 1280], P(('dp', 'sp')), parts along dimension 0
There are 2 independent parts. The reference program is written for one: setup_inputs(seed, part) draws one part's arguments, and reference() takes and returns one part's arrays. A program takes and returns all parts, laid end to end along the dimension named above; an argument that names none is the same for every part.
All inputs are finite; a program needn't handle non-finite values.
Results may differ from the reference program's by a relative error of at most 0.0133211.
Values are sent between devices in bfloat16 or wider.
A program may use at most 1 GiB of HBM per device.

```python
import jax
import jax.numpy as jnp
from jax import lax

SHARDS = 4
TQ_DEV = 512
TM_DEV = 512
D_MODEL = 1280
HEAD = 64
KV_HEADS = 1
FF_DIM = 5120
LAYERS = 2

TQ_LEN = TQ_DEV * SHARDS
TM_LEN = TM_DEV * SHARDS
HEADS = D_MODEL // HEAD
KV_DIM = HEAD * KV_HEADS
GROUP_SIZE = HEADS // KV_HEADS
ATT_SCALE = HEAD ** -0.5


def draw_matrix(key_mat, shape):
    return (jax.random.normal(key_mat, shape, jnp.float32) * shape[1] ** -0.5).astype(jnp.bfloat16)


def draw_gain(key_gain):
    return (1.0 + 0.3 * jax.random.normal(key_gain, (LAYERS, D_MODEL), jnp.float32)).astype(jnp.bfloat16)


def setup_inputs(seed: int = 0, part: int = 0) -> dict:
    part_key = jax.random.fold_in(jax.random.key(seed), part)
    part_keys = jax.random.split(part_key, 5)
    dec_noise = jax.random.normal(part_keys[0], (SHARDS, TQ_DEV, D_MODEL), jnp.float32)
    dec_shift = 0.8 * jax.random.normal(part_keys[1], (SHARDS, 1, D_MODEL), jnp.float32)
    mem_noise = jax.random.normal(part_keys[2], (SHARDS, TM_DEV, D_MODEL), jnp.float32)
    mem_shift = jax.random.normal(part_keys[3], (SHARDS, 1, D_MODEL), jnp.float32)
    mem_len = jax.random.randint(part_keys[4], (1,), TM_LEN // 4 + 1, 3 * TM_LEN // 4 + 1, dtype=jnp.int32)
    w_keys = jax.random.split(jax.random.key(seed + 1), 14)
    return {
        "dec_hidden": (dec_noise + dec_shift).reshape(TQ_LEN, D_MODEL).astype(jnp.bfloat16),
        "memory": (mem_noise + mem_shift).reshape(TM_LEN, D_MODEL).astype(jnp.bfloat16),
        "mem_len": mem_len,
        "gain_self": draw_gain(w_keys[0]),
        "gain_cross": draw_gain(w_keys[1]),
        "gain_mlp": draw_gain(w_keys[2]),
        "self_q": draw_matrix(w_keys[3], (LAYERS, D_MODEL, D_MODEL)),
        "self_k": draw_matrix(w_keys[4], (LAYERS, D_MODEL, D_MODEL)),
        "self_v": draw_matrix(w_keys[5], (LAYERS, D_MODEL, D_MODEL)),
        "self_o": draw_matrix(w_keys[6], (LAYERS, D_MODEL, D_MODEL)),
        "cross_q": draw_matrix(w_keys[7], (LAYERS, D_MODEL, D_MODEL)),
        "cross_k": draw_matrix(w_keys[8], (LAYERS, D_MODEL, KV_DIM)),
        "cross_v": draw_matrix(w_keys[9], (LAYERS, D_MODEL, KV_DIM)),
        "cross_o": draw_matrix(w_keys[10], (LAYERS, D_MODEL, D_MODEL)),
        "mlp_gate": draw_matrix(w_keys[11], (LAYERS, D_MODEL, FF_DIM)),
        "mlp_up": draw_matrix(w_keys[12], (LAYERS, D_MODEL, FF_DIM)),
        "mlp_down": draw_matrix(w_keys[13], (LAYERS, FF_DIM, D_MODEL)),
    }


def rms_norm(values, gain_vec):
    val32 = values.astype(jnp.float32)
    inv_rms = lax.rsqrt(jnp.mean(val32 * val32, axis=-1, keepdims=True) + 1e-6)
    return (val32 * inv_rms * gain_vec.astype(jnp.float32)).astype(jnp.bfloat16)


def project(rows, weight):
    return jnp.dot(rows, weight, preferred_element_type=jnp.float32)


def add_residual(hidden, update):
    return (hidden.astype(jnp.float32) + update).astype(jnp.bfloat16)


def head_attend(q_head, k_head, v_head, valid):
    scores = jnp.dot(q_head, k_head.T, preferred_element_type=jnp.float32) * ATT_SCALE
    scores = jnp.where(valid, scores, -1e30)
    row_max = jnp.max(scores, axis=1, keepdims=True)
    exp_vals = jnp.exp(scores - row_max)
    row_sum = jnp.sum(exp_vals, axis=1, keepdims=True)
    weighted = jnp.dot(exp_vals.astype(jnp.bfloat16), v_head, preferred_element_type=jnp.float32)
    return weighted / row_sum


def multi_head(q_rows, k_rows, v_rows, valid, group_size):
    q_len = q_rows.shape[0]
    k_len = k_rows.shape[0]
    q_heads = q_rows.reshape(q_len, HEADS, HEAD).transpose(1, 0, 2)
    k_heads = k_rows.reshape(k_len, -1, HEAD).transpose(1, 0, 2)
    v_heads = v_rows.reshape(k_len, -1, HEAD).transpose(1, 0, 2)

    def one_head(head_idx):
        kv_idx = head_idx // group_size
        return head_attend(q_heads[head_idx], k_heads[kv_idx], v_heads[kv_idx], valid)

    per_head = lax.map(one_head, jnp.arange(HEADS))
    return per_head.transpose(1, 0, 2).reshape(q_len, HEADS * HEAD).astype(jnp.bfloat16)


def reference(dec_hidden, memory, mem_len, gain_self, gain_cross, gain_mlp, self_q, self_k, self_v, self_o, cross_q, cross_k, cross_v, cross_o, mlp_gate, mlp_up, mlp_down):
    positions = jnp.arange(TQ_LEN)
    causal = positions[:, None] >= positions[None, :]
    mem_valid = (jnp.arange(TM_LEN) < mem_len[0])[None, :]

    def decoder_layer(hidden, layer_w):
        (g_self, g_cross, g_mlp, w_query, w_key, w_value, w_out, x_query, x_key, x_value, x_out, w_gate, w_up, w_down) = layer_w
        normed = rms_norm(hidden, g_self)
        q_rows = project(normed, w_query).astype(jnp.bfloat16)
        k_rows = project(normed, w_key).astype(jnp.bfloat16)
        v_rows = project(normed, w_value).astype(jnp.bfloat16)
        attn_out = multi_head(q_rows, k_rows, v_rows, causal, 1)
        hidden = add_residual(hidden, project(attn_out, w_out))
        normed = rms_norm(hidden, g_cross)
        q_rows = project(normed, x_query).astype(jnp.bfloat16)
        mem_k = project(memory, x_key).astype(jnp.bfloat16)
        mem_v = project(memory, x_value).astype(jnp.bfloat16)
        attn_out = multi_head(q_rows, mem_k, mem_v, mem_valid, GROUP_SIZE)
        hidden = add_residual(hidden, project(attn_out, x_out))
        normed = rms_norm(hidden, g_mlp)
        act_vals = (jax.nn.silu(project(normed, w_gate)) * project(normed, w_up)).astype(jnp.bfloat16)
        hidden = add_residual(hidden, project(act_vals, w_down))
        return hidden, None

    weights = (gain_self, gain_cross, gain_mlp, self_q, self_k, self_v, self_o, cross_q, cross_k, cross_v, cross_o, mlp_gate, mlp_up, mlp_down)
    return lax.scan(decoder_layer, dec_hidden, weights)[0]
```

```python
import functools

import jax
import jax.numpy as jnp
from jax import lax
from jax.experimental import pallas as pl
from jax.experimental.pallas import tpu as pltpu
from jax.sharding import PartitionSpec as P

HEAD = 64
EPS = 1e-6
MASK = -1e30
EXP_SCALE = (HEAD ** -0.5) * 1.4426950408889634
MIB = 1024 * 1024
F32 = jnp.float32
BF16 = jnp.bfloat16


def norm_rows(values, gain_row):
    val32 = values.astype(F32)
    inv_rms = lax.rsqrt(jnp.mean(val32 * val32, axis=-1, keepdims=True) + EPS)
    return (val32 * inv_rms * gain_row.astype(F32)).astype(BF16)


def dot32(left, right):
    return jnp.dot(left, right, preferred_element_type=F32)


def scores_of(k_blk, q_blk, keep):
    scores = dot32(k_blk, q_blk)
    if keep is not None:
        scores = jnp.where(keep, scores, MASK)
    return scores


def soft_first(scores, v_blk):
    top = jnp.max(scores, axis=0, keepdims=True)
    exps = jnp.exp2(scores * EXP_SCALE - top * EXP_SCALE)
    total = jnp.sum(exps, axis=0, keepdims=True)
    return top, total, dot32(v_blk, exps.astype(BF16))


def soft_next(state, scores, v_blk):
    top_old, total_old, acc_old = state
    top = jnp.maximum(top_old, jnp.max(scores, axis=0, keepdims=True))
    decay = jnp.exp2((top_old - top) * EXP_SCALE)
    exps = jnp.exp2(scores * EXP_SCALE - top * EXP_SCALE)
    total = total_old * decay + jnp.sum(exps, axis=0, keepdims=True)
    return top, total, acc_old * decay + dot32(v_blk, exps.astype(BF16))


def qkv_kernel(n_out, layer, meta, x0, x1, gain, *refs):
    weights, outs = refs[:n_out], refs[n_out:]
    for slot, x_ref in enumerate((x0, x1)):
        normed = norm_rows(x_ref[...], gain[layer:layer + 1, :])
        for idx in range(n_out):
            rows = dot32(normed, weights[idx][0]).astype(BF16)
            if n_out - idx == 2:
                outs[idx][slot] = rows
            else:
                outs[idx][slot] = rows.T


def qkv_call(meta, x0, x1, gain, weights, layer):
    rows, d_model = x0.shape
    half = d_model // 2
    n_out = len(weights)
    out_shape, out_specs = [], []
    for idx in range(n_out):
        shape = (2, rows, half) if n_out - idx == 2 else (2, half, rows)
        out_shape.append(jax.ShapeDtypeStruct(shape, BF16))
        out_specs.append(pl.BlockSpec(shape, lambda i, m: (0, 0, 0)))
    full = lambda shape: pl.BlockSpec(shape, lambda i, m: (0,) * len(shape))
    return pl.pallas_call(
        functools.partial(qkv_kernel, n_out, layer),
        grid_spec=pltpu.PrefetchScalarGridSpec(
            num_scalar_prefetch=1,
            grid=(1,),
            in_specs=[full(x0.shape), full(x1.shape), full(gain.shape)]
            + [pl.BlockSpec((1, d_model, half), lambda i, m: (layer, 0, m[1]))] * n_out,
            out_specs=out_specs,
        ),
        out_shape=out_shape,
        compiler_params=pltpu.CompilerParams(vmem_limit_bytes=60 * MIB),
        cost_estimate=pl.CostEstimate(flops=2 * 2 * rows * d_model * half * n_out, bytes_accessed=10 * MIB, transcendentals=0),
        name="qkv" if n_out == 3 else "kv_remote",
    )(meta, x0, x1, gain, *weights)


def self_kernel(meta, q_ref, k_ref, v_ref, kr_ref, vr_ref, own_ref, send_ref, top_s, tot_s, acc_s):
    core, chip = meta[1], meta[0]
    rows = k_ref.shape[1]
    pad = jnp.zeros((HEAD, rows), BF16)
    tri = lax.broadcasted_iota(jnp.int32, (rows, rows), 0) <= lax.broadcasted_iota(jnp.int32, (rows, rows), 1)

    def q_of(half, head):
        q_head = q_ref[half ^ core, head * HEAD:(head + 1) * HEAD, :]
        return jnp.concatenate([q_head, pad] if head == 0 else [pad, q_head], axis=0)

    def v_of(ref, slot, head):
        return ref[slot, head * HEAD:(head + 1) * HEAD, :]

    for half in range(2):
        for head in range(2):
            q_blk = q_of(half, head)
            state = soft_first(scores_of(k_ref[half ^ core], q_blk, tri), v_of(v_ref, half ^ core, head))
            if half == 1:
                state = soft_next(state, scores_of(k_ref[core], q_blk, None), v_of(v_ref, core, head))
            idx = 2 * half + head
            top_s[idx], tot_s[idx], acc_s[idx] = state

    @pl.when(chip == 1)
    def remote():
        for half in range(2):
            for head in range(2):
                idx = 2 * half + head
                q_blk = q_of(half, head)
                state = top_s[idx], tot_s[idx], acc_s[idx]
                for slot in range(2):
                    state = soft_next(state, scores_of(kr_ref[slot], q_blk, None), v_of(vr_ref, slot, head))
                top_s[idx], tot_s[idx], acc_s[idx] = state

    for slot, out in enumerate((own_ref, send_ref)):
        for head in range(2):
            idx = 2 * (slot ^ core) + head
            out[head * HEAD:(head + 1) * HEAD, :] = (acc_s[idx] / tot_s[idx]).astype(BF16)


def self_call(meta, q_t, k_rows, v_t, kr_rows, vr_t):
    half, rows = q_t.shape[1], q_t.shape[2]
    pair = 2 * HEAD
    feat = pl.BlockSpec((2, pair, rows), lambda i, m: (0, i, 0))
    keys = pl.BlockSpec((2, rows, pair), lambda i, m: (0, 0, i))
    out = jax.ShapeDtypeStruct((half, rows), BF16)
    return pl.pallas_call(
        self_kernel,
        grid_spec=pltpu.PrefetchScalarGridSpec(
            num_scalar_prefetch=1,
            grid=(half // pair,),
            in_specs=[feat, keys, feat, keys, feat],
            out_specs=[pl.BlockSpec((pair, rows), lambda i, m: (i, 0))] * 2,
            scratch_shapes=[pltpu.VMEM((4, 1, rows), F32), pltpu.VMEM((4, 1, rows), F32), pltpu.VMEM((4, HEAD, rows), F32)],
        ),
        out_shape=[out, out],
        compiler_params=pltpu.CompilerParams(vmem_limit_bytes=60 * MIB),
        cost_estimate=pl.CostEstimate(flops=8 * 2 * 2 * rows * rows * half * 2, bytes_accessed=10 * MIB, transcendentals=0),
        name="self_attn",
    )(meta, q_t, k_rows, v_t, kr_rows, vr_t)


def mid_kernel(layer, meta, y_ref, own_ref, recv_ref, gain, wo, wxq, wxo, kx_ref, vx_ref, out_ref, q_s, o_s):
    shard, core, mem_len = meta[2], meta[1], meta[3]
    d_model = y_ref.shape[1]
    rows = y_ref.shape[0]
    half = d_model // 2
    upd = dot32(own_ref[...].T, wo[0, pl.ds(core * half, half), :])
    upd += dot32(recv_ref[...].T, wo[0, pl.ds((1 - core) * half, half), :])
    y1 = (y_ref[...].astype(F32) + upd).astype(BF16)
    normed = norm_rows(y1, gain[layer:layer + 1, :])
    q_s[...] = dot32(normed, wxq[0]).astype(BF16).T
    n_heads = d_model // HEAD
    key_pos = lax.broadcasted_iota(jnp.int32, (rows, rows), 0)

    def head_group(base):
        for off in range(2):
            row = pl.multiple_of((base * 2 + off) * HEAD, HEAD)
            q_blk = q_s[pl.ds(row, HEAD), :]
            state = soft_first(scores_of(kx_ref[shard], q_blk, None), vx_ref[shard])
            keep = key_pos < mem_len - rows
            state = soft_next(state, scores_of(kx_ref[1 ^ shard], q_blk, keep), vx_ref[1 ^ shard])
            keep = key_pos < mem_len - 2 * rows
            state = soft_next(state, scores_of(kx_ref[2 ^ shard], q_blk, keep), vx_ref[2 ^ shard])
            o_s[pl.ds(row, HEAD), :] = (state[2] / state[1]).astype(BF16)

    pl.loop(0, n_heads // 2)(head_group)
    out_ref[...] = (y1.astype(F32) + dot32(o_s[...].T, wxo[0])).astype(BF16)


def mid_call(meta, y, o_own, o_recv, gain, wo, wxq, wxo, kx, vx, layer):
    rows, d_model = y.shape
    full = lambda shape: pl.BlockSpec(shape, lambda i, m: (0,) * len(shape))
    weight = pl.BlockSpec((1, d_model, d_model), lambda i, m: (layer, 0, 0))
    return pl.pallas_call(
        functools.partial(mid_kernel, layer),
        grid_spec=pltpu.PrefetchScalarGridSpec(
            num_scalar_prefetch=1,
            grid=(1,),
            in_specs=[full(y.shape), full(o_own.shape), full(o_recv.shape), full(gain.shape), weight, weight, weight,
                      full(kx.shape), full(vx.shape)],
            out_specs=full(y.shape),
            scratch_shapes=[pltpu.VMEM((d_model, rows), BF16), pltpu.VMEM((d_model, rows), BF16)],
        ),
        out_shape=jax.ShapeDtypeStruct(y.shape, BF16),
        compiler_params=pltpu.CompilerParams(vmem_limit_bytes=60 * MIB),
        cost_estimate=pl.CostEstimate(flops=3 * 2 * rows * d_model * d_model + 2 * 2 * rows * 1536 * d_model, bytes_accessed=14 * MIB, transcendentals=0),
        name="mid",
    )(meta, y, o_own, o_recv, gain, wo, wxq, wxo, kx, vx)


def mlp_kernel(layer, y_ref, gain, wg, wu, wd, out_ref, h_s, acc_s):
    step = pl.program_id(0)

    @pl.when(step == 0)
    def first():
        h_s[...] = norm_rows(y_ref[...], gain[layer:layer + 1, :])
        acc_s[...] = y_ref[...].astype(F32) * 0.0

    normed = h_s[...]
    gate = dot32(normed, wg[0])
    acts = (jax.nn.silu(gate) * dot32(normed, wu[0])).astype(BF16)
    acc_s[...] += dot32(acts, wd[0])

    @pl.when(step == pl.num_programs(0) - 1)
    def last():
        out_ref[...] = (y_ref[...].astype(F32) + acc_s[...]).astype(BF16)


def mlp_call(y, gain, wg, wu, wd, layer):
    rows, d_model = y.shape
    ff = wg.shape[2]
    tile = 512
    full = lambda shape: pl.BlockSpec(shape, lambda i: (0,) * len(shape))
    return pl.pallas_call(
        functools.partial(mlp_kernel, layer),
        grid=(ff // tile,),
        in_specs=[full(y.shape), full(gain.shape),
                  pl.BlockSpec((1, d_model, tile), lambda i: (layer, 0, i)),
                  pl.BlockSpec((1, d_model, tile), lambda i: (layer, 0, i)),
                  pl.BlockSpec((1, tile, d_model), lambda i: (layer, i, 0))],
        out_specs=full(y.shape),
        scratch_shapes=[pltpu.VMEM((rows, d_model), BF16), pltpu.VMEM((rows, d_model), F32)],
        out_shape=jax.ShapeDtypeStruct(y.shape, BF16),
        compiler_params=pltpu.CompilerParams(vmem_limit_bytes=60 * MIB),
        cost_estimate=pl.CostEstimate(flops=3 * 2 * rows * d_model * ff, bytes_accessed=40 * MIB, transcendentals=rows * ff),
        name="mlp",
    )(y, gain, wg, wu, wd)


SWAP = [(0, 1), (1, 0), (2, 3), (3, 2)]
CROSS = [(0, 2), (1, 3)]


def solution(mesh):
    row_spec = P(("dp", "sp"), None)

    def device_fn(dec_hidden, memory, mem_len, gain_self, gain_cross, gain_mlp, self_q, self_k, self_v, self_o, cross_q, cross_k, cross_v, cross_o, mlp_gate, mlp_up, mlp_down):
        n_layers = gain_self.shape[0]
        shard = lax.axis_index("sp").astype(jnp.int32)
        meta = jnp.stack([shard // 2, shard % 2, shard, mem_len[0]])

        kv_w = jnp.concatenate([cross_k[0], cross_k[1], cross_v[0], cross_v[1]], axis=1)
        kv_own = dot32(memory, kv_w).astype(BF16)
        kv_all = jnp.stack([kv_own] + [lax.ppermute(kv_own, "sp", [(i, i ^ d) for i in range(4)]) for d in (1, 2, 3)])

        hidden = dec_hidden
        for layer in range(n_layers):
            other = lax.ppermute(hidden, "sp", SWAP)
            remote0 = lax.ppermute(hidden, "sp", CROSS)
            remote1 = lax.ppermute(remote0, "sp", SWAP)
            q_t, k_rows, v_t = qkv_call(meta, hidden, other, gain_self, (self_q, self_k, self_v), layer)
            kr_rows, vr_t = qkv_call(meta, remote0, remote1, gain_self, (self_k, self_v), layer)
            o_own, o_send = self_call(meta, q_t, k_rows, v_t, kr_rows, vr_t)
            o_recv = lax.ppermute(o_send, "sp", SWAP)
            kx = kv_all[:, :, layer * HEAD:(layer + 1) * HEAD]
            vx = kv_all[:, :, (2 + layer) * HEAD:(3 + layer) * HEAD].transpose(0, 2, 1)
            hidden = mid_call(meta, hidden, o_own, o_recv, gain_cross, self_o, cross_q, cross_o, kx, vx, layer)
            hidden = mlp_call(hidden, gain_mlp, mlp_gate, mlp_up, mlp_down, layer)
        return hidden

    return jax.shard_map(device_fn, mesh=mesh, in_specs=(row_spec, row_spec, P("dp")) + (P(),) * 14, out_specs=row_spec, check_vma=False)
```

```python
import functools

import jax
import jax.numpy as jnp
from jax import lax
from jax.experimental import pallas as pl
from jax.experimental.pallas import tpu as pltpu
from jax.sharding import PartitionSpec as P

HEAD = 64
EPS = 1e-6
MASK = -1e30
EXP_SCALE = (HEAD ** -0.5) * 1.4426950408889634
MIB = 1024 * 1024
F32 = jnp.float32
BF16 = jnp.bfloat16


def norm_rows(values, gain_row):
    val32 = values.astype(F32)
    inv_rms = lax.rsqrt(jnp.mean(val32 * val32, axis=-1, keepdims=True) + EPS)
    return (val32 * inv_rms * gain_row.astype(F32)).astype(BF16)


def dot32(left, right):
    return jnp.dot(left, right, preferred_element_type=F32)


SUB = 128


def fold8(values, op):
    parts = values.reshape(values.shape[0] // 8, 8, values.shape[1])
    return op(parts, axis=0)


def attend(items, s_bufs, p_bufs):
    n_items = len(items)
    states, tops, work = {}, {}, {}
    for t in range(n_items + 2):
        if t < n_items:
            k_of, q_rhs, _, keep_of, _, n_keys = items[t]
            top8 = None
        if 1 <= t <= n_items:
            _, _, _, _, chain, n_keys_b = items[t - 1]
            top = jnp.max(tops[t - 1], axis=0, keepdims=True)
            decay = None
            if chain in states:
                top_old, total_old = states[chain][:2]
                top = jnp.maximum(top_old, top)
                decay = jnp.exp2((top_old - top) * EXP_SCALE)
            shift = top * EXP_SCALE
            total8 = None
        n_sub = max(items[u][5] for u in (t, t - 1, t - 2) if 0 <= u < n_items) // SUB
        acc_new = None
        for sub in range(n_sub):
            if t < n_items and sub * SUB < n_keys:
                scores = dot32(k_of(sub * SUB, SUB), q_rhs)
                if keep_of is not None:
                    scores = jnp.where(keep_of(sub * SUB, SUB), scores, MASK)
                s_bufs[t % 2][sub * SUB:(sub + 1) * SUB, :] = scores
                part = fold8(scores, jnp.max)
                top8 = part if top8 is None else jnp.maximum(top8, part)
            if 1 <= t <= n_items and sub * SUB < n_keys_b:
                exps = jnp.exp2(s_bufs[(t - 1) % 2][sub * SUB:(sub + 1) * SUB, :] * EXP_SCALE - shift)
                part = fold8(exps, jnp.sum)
                total8 = part if total8 is None else total8 + part
                p_bufs[(t - 1) % 2][sub * SUB:(sub + 1) * SUB, :] = exps.astype(BF16)
            if t >= 2 and sub % 2 == 1 and (sub + 1) * SUB <= items[t - 2][5]:
                row0 = (sub - 1) * SUB
                part = dot32(items[t - 2][2](row0, 2 * SUB), p_bufs[t % 2][row0:row0 + 2 * SUB, :])
                acc_new = part if acc_new is None else acc_new + part
        if t < n_items:
            tops[t] = top8
        if t >= 2:
            chain = items[t - 2][4]
            decay_c = work.pop(t - 2)
            old = states[chain][2]
            states[chain] = states[chain][:2] + (acc_new if old is None else old * decay_c + acc_new,)
        if 1 <= t <= n_items:
            if decay is not None:
                total8 = total_old * decay + total8
            states[chain_of(items, t - 1)] = (top, total8, states.get(chain_of(items, t - 1), (None, None, None))[2])
            work[t - 1] = decay
    return states


def chain_of(items, t):
    return items[t][4]


def qkv_kernel(n_out, layer, meta, x0, x1, gain, *refs):
    weights, outs = refs[:n_out], refs[n_out:]
    for slot, x_ref in enumerate((x0, x1)):
        normed = norm_rows(x_ref[...], gain[layer:layer + 1, :])
        for idx in range(n_out):
            rows = dot32(normed, weights[idx][0]).astype(BF16)
            if n_out - idx == 2:
                outs[idx][slot] = rows
            else:
                outs[idx][slot] = rows.T


def qkv_call(meta, x0, x1, gain, weights, layer):
    rows, d_model = x0.shape
    half = d_model // 2
    n_out = len(weights)
    out_shape, out_specs = [], []
    for idx in range(n_out):
        shape = (2, rows, half) if n_out - idx == 2 else (2, half, rows)
        out_shape.append(jax.ShapeDtypeStruct(shape, BF16))
        out_specs.append(pl.BlockSpec(shape, lambda i, m: (0, 0, 0)))
    full = lambda shape: pl.BlockSpec(shape, lambda i, m: (0,) * len(shape))
    return pl.pallas_call(
        functools.partial(qkv_kernel, n_out, layer),
        grid_spec=pltpu.PrefetchScalarGridSpec(
            num_scalar_prefetch=1,
            grid=(1,),
            in_specs=[full(x0.shape), full(x1.shape), full(gain.shape)]
            + [pl.BlockSpec((1, d_model, half), lambda i, m: (layer, 0, m[1]))] * n_out,
            out_specs=out_specs,
        ),
        out_shape=out_shape,
        compiler_params=pltpu.CompilerParams(vmem_limit_bytes=60 * MIB),
        cost_estimate=pl.CostEstimate(flops=2 * 2 * rows * d_model * half * n_out, bytes_accessed=10 * MIB, transcendentals=0),
        name="qkv" if n_out == 3 else "kv_remote",
    )(meta, x0, x1, gain, *weights)


def self_kernel(meta, q_ref, k_ref, v_ref, kr_ref, vr_ref, own_ref, send_ref, s0, s1, p0, p1, top_s, tot_s, acc_s):
    core, chip = meta[1], meta[0]
    rows = k_ref.shape[1]
    pad = jnp.zeros((HEAD, rows), BF16)

    def q_of(half, head):
        q_head = q_ref[half ^ core, head * HEAD:(head + 1) * HEAD, :]
        return jnp.concatenate([q_head, pad] if head == 0 else [pad, q_head], axis=0)

    def item(k_r, v_r, slot, half, head, diag):
        def keep_of(row0, n):
            key = lax.broadcasted_iota(jnp.int32, (n, rows), 0) + row0
            return key <= lax.broadcasted_iota(jnp.int32, (n, rows), 1)

        return (lambda row0, n: k_r[slot, row0:row0 + n, :], q_of(half, head),
                lambda row0, n: v_r[slot, head * HEAD:(head + 1) * HEAD, row0:row0 + n],
                keep_of if diag else None, (half, head), rows)

    def finish(states):
        for (half, head), (top, tot, acc) in states.items():
            tot = jnp.sum(tot, axis=0, keepdims=True)
            idx = 2 * (half ^ core) + head
            acc_s[idx] = acc / tot

    local = []
    for head in range(2):
        local.append(item(k_ref, v_ref, core, 0, head, True))
        local.append(item(k_ref, v_ref, core, 1, head, False))
        local.append(item(k_ref, v_ref, 1 ^ core, 1, head, True))
    local = [local[i] for i in (0, 1, 3, 4, 2, 5)]

    @pl.when(chip == 0)
    def first_chip():
        finish(attend(local, (s0, s1), (p0, p1)))

    @pl.when(chip == 1)
    def second_chip():
        remote = [item(kr_ref, vr_ref, slot, half, head, False) for slot in range(2) for half in range(2) for head in range(2)]
        finish(attend(local + remote, (s0, s1), (p0, p1)))

    for slot, out in enumerate((own_ref, send_ref)):
        for head in range(2):
            out[head * HEAD:(head + 1) * HEAD, :] = acc_s[2 * slot + head].astype(BF16)


def self_call(meta, q_t, k_rows, v_t, kr_rows, vr_t):
    half, rows = q_t.shape[1], q_t.shape[2]
    pair = 2 * HEAD
    feat = pl.BlockSpec((2, pair, rows), lambda i, m: (0, i, 0))
    keys = pl.BlockSpec((2, rows, pair), lambda i, m: (0, 0, i))
    out = jax.ShapeDtypeStruct((half, rows), BF16)
    return pl.pallas_call(
        self_kernel,
        grid_spec=pltpu.PrefetchScalarGridSpec(
            num_scalar_prefetch=1,
            grid=(half // pair,),
            in_specs=[feat, keys, feat, keys, feat],
            out_specs=[pl.BlockSpec((pair, rows), lambda i, m: (i, 0))] * 2,
            scratch_shapes=[pltpu.VMEM((rows, rows), F32)] * 2 + [pltpu.VMEM((rows, rows), BF16)] * 2
            + [pltpu.VMEM((4, 1, rows), F32), pltpu.VMEM((4, 1, rows), F32), pltpu.VMEM((4, HEAD, rows), F32)],
        ),
        out_shape=[out, out],
        compiler_params=pltpu.CompilerParams(vmem_limit_bytes=60 * MIB),
        cost_estimate=pl.CostEstimate(flops=8 * 2 * 2 * rows * rows * half * 2, bytes_accessed=10 * MIB, transcendentals=0),
        name="self_attn",
    )(meta, q_t, k_rows, v_t, kr_rows, vr_t)


def mid_kernel(layer, meta, y_ref, own_ref, recv_ref, gain, wo, wxq, wxo, kx_ref, vx_ref, out_ref, q_s, o_s, s0, s1, p0, p1):
    shard, core, mem_len = meta[2], meta[1], meta[3]
    d_model = y_ref.shape[1]
    rows = y_ref.shape[0]
    half = d_model // 2
    upd = dot32(own_ref[...].T, wo[0, pl.ds(core * half, half), :])
    upd += dot32(recv_ref[...].T, wo[0, pl.ds((1 - core) * half, half), :])
    y1 = (y_ref[...].astype(F32) + upd).astype(BF16)
    normed = norm_rows(y1, gain[layer:layer + 1, :])
    q_s[...] = dot32(normed, wxq[0]).astype(BF16).T
    n_heads = d_model // HEAD

    def heads_loop(n_blocks):
        def head_group(base):
            items = []
            rows_of = [pl.multiple_of((base * 4 + off) * HEAD, HEAD) for off in range(4)]
            q_vals = [q_s[pl.ds(row, HEAD), :] for row in rows_of]
            for blk in range(n_blocks):
                for off in range(4):
                    def keep_of(row0, n, blk=blk):
                        return lax.broadcasted_iota(jnp.int32, (n, rows), 0) + row0 < mem_len - blk * rows

                    items.append((lambda row0, n, blk=blk: kx_ref[blk ^ shard, row0:row0 + n, :], q_vals[off],
                                  lambda row0, n, blk=blk: vx_ref[blk ^ shard, :, row0:row0 + n],
                                  keep_of if blk == n_blocks - 1 else None, off, rows))
            for off, (top, tot, acc) in attend(items, (s0, s1), (p0, p1)).items():
                o_s[pl.ds(rows_of[off], HEAD), :] = (acc / jnp.sum(tot, axis=0, keepdims=True)).astype(BF16)

        pl.loop(0, n_heads // 4)(head_group)

    @pl.when(mem_len <= 2 * rows)
    def short():
        heads_loop(2)

    @pl.when(mem_len > 2 * rows)
    def long():
        heads_loop(3)

    out_ref[...] = (y1.astype(F32) + dot32(o_s[...].T, wxo[0])).astype(BF16)


def mid_call(meta, y, o_own, o_recv, gain, wo, wxq, wxo, kx, vx, layer):
    rows, d_model = y.shape
    full = lambda shape: pl.BlockSpec(shape, lambda i, m: (0,) * len(shape))
    weight = pl.BlockSpec((1, d_model, d_model), lambda i, m: (layer, 0, 0))
    return pl.pallas_call(
        functools.partial(mid_kernel, layer),
        grid_spec=pltpu.PrefetchScalarGridSpec(
            num_scalar_prefetch=1,
            grid=(1,),
            in_specs=[full(y.shape), full(o_own.shape), full(o_recv.shape), full(gain.shape), weight, weight, weight,
                      full(kx.shape), full(vx.shape)],
            out_specs=full(y.shape),
            scratch_shapes=[pltpu.VMEM((d_model, rows), BF16), pltpu.VMEM((d_model, rows), BF16)]
            + [pltpu.VMEM((rows, rows), F32)] * 2 + [pltpu.VMEM((rows, rows), BF16)] * 2,
        ),
        out_shape=jax.ShapeDtypeStruct(y.shape, BF16),
        compiler_params=pltpu.CompilerParams(vmem_limit_bytes=60 * MIB),
        cost_estimate=pl.CostEstimate(flops=3 * 2 * rows * d_model * d_model + 2 * 2 * rows * 1536 * d_model, bytes_accessed=14 * MIB, transcendentals=0),
        name="mid",
    )(meta, y, o_own, o_recv, gain, wo, wxq, wxo, kx, vx)


def mlp_kernel(layer, y_ref, gain, wg, wu, wd, out_ref, h_s, acc_s):
    step = pl.program_id(0)

    @pl.when(step == 0)
    def first():
        h_s[...] = norm_rows(y_ref[...], gain[layer:layer + 1, :])
        acc_s[...] = y_ref[...].astype(F32) * 0.0

    normed = h_s[...]
    gate = dot32(normed, wg[0])
    acts = (jax.nn.silu(gate) * dot32(normed, wu[0])).astype(BF16)
    acc_s[...] += dot32(acts, wd[0])

    @pl.when(step == pl.num_programs(0) - 1)
    def last():
        out_ref[...] = (y_ref[...].astype(F32) + acc_s[...]).astype(BF16)


def mlp_call(y, gain, wg, wu, wd, layer):
    rows, d_model = y.shape
    ff = wg.shape[2]
    tile = 512
    full = lambda shape: pl.BlockSpec(shape, lambda i: (0,) * len(shape))
    return pl.pallas_call(
        functools.partial(mlp_kernel, layer),
        grid=(ff // tile,),
        in_specs=[full(y.shape), full(gain.shape),
                  pl.BlockSpec((1, d_model, tile), lambda i: (layer, 0, i)),
                  pl.BlockSpec((1, d_model, tile), lambda i: (layer, 0, i)),
                  pl.BlockSpec((1, tile, d_model), lambda i: (layer, i, 0))],
        out_specs=full(y.shape),
        scratch_shapes=[pltpu.VMEM((rows, d_model), BF16), pltpu.VMEM((rows, d_model), F32)],
        out_shape=jax.ShapeDtypeStruct(y.shape, BF16),
        compiler_params=pltpu.CompilerParams(vmem_limit_bytes=60 * MIB),
        cost_estimate=pl.CostEstimate(flops=3 * 2 * rows * d_model * ff, bytes_accessed=40 * MIB, transcendentals=rows * ff),
        name="mlp",
    )(y, gain, wg, wu, wd)


SWAP = [(0, 1), (1, 0), (2, 3), (3, 2)]
CROSS = [(0, 2), (1, 3)]


def solution(mesh):
    row_spec = P(("dp", "sp"), None)

    def device_fn(dec_hidden, memory, mem_len, gain_self, gain_cross, gain_mlp, self_q, self_k, self_v, self_o, cross_q, cross_k, cross_v, cross_o, mlp_gate, mlp_up, mlp_down):
        n_layers = gain_self.shape[0]
        shard = lax.axis_index("sp").astype(jnp.int32)
        meta = jnp.stack([shard // 2, shard % 2, shard, mem_len[0]])

        kv_w = jnp.concatenate([cross_k[0], cross_k[1], cross_v[0], cross_v[1]], axis=1)
        kv_own = dot32(memory, kv_w).astype(BF16)
        kv_all = jnp.stack([kv_own] + [lax.ppermute(kv_own, "sp", [(i, i ^ d) for i in range(4)]) for d in (1, 2, 3)])

        hidden = dec_hidden
        for layer in range(n_layers):
            other = lax.ppermute(hidden, "sp", SWAP)
            remote0 = lax.ppermute(hidden, "sp", CROSS)
            remote1 = lax.ppermute(remote0, "sp", SWAP)
            q_t, k_rows, v_t = qkv_call(meta, hidden, other, gain_self, (self_q, self_k, self_v), layer)
            kr_rows, vr_t = qkv_call(meta, remote0, remote1, gain_self, (self_k, self_v), layer)
            o_own, o_send = self_call(meta, q_t, k_rows, v_t, kr_rows, vr_t)
            o_recv = lax.ppermute(o_send, "sp", SWAP)
            kx = kv_all[:, :, layer * HEAD:(layer + 1) * HEAD]
            vx = kv_all[:, :, (2 + layer) * HEAD:(3 + layer) * HEAD].transpose(0, 2, 1)
            hidden = mid_call(meta, hidden, o_own, o_recv, gain_cross, self_o, cross_q, cross_o, kx, vx, layer)
            hidden = mlp_call(hidden, gain_mlp, mlp_gate, mlp_up, mlp_down, layer)
        return hidden

    return jax.shard_map(device_fn, mesh=mesh, in_specs=(row_spec, row_spec, P("dp")) + (P(),) * 14, out_specs=row_spec, check_vma=False)
```
